32 devices in a mesh: row: 16 (over z, x, core), feat: 2 (over y).
Axes of the slice: x: 2, y: 2, z: 4, core: 2. Of those that a mesh axis runs over, the one named last changes fastest.
Arguments:
- bin_index: int32 [1024, 49152], P('feat', 'row'), may hold values from 0 to 63
- gradient: bfloat16 [32, 49152], P(None, ('row', 'feat')), may hold values from -6 to 6
- hessian: bfloat16 [49152], P(('row', 'feat')), may hold values from 0.25 to 4
- row_node: int32 [49152], P('row'), may hold values from 0 to 7
Outputs:
- split_gain: float32 [1024, 512], P(('feat', 'row'))
- best_gain: float32 [8], replicated
The draws below stay inside these ranges and needn't reach their ends.
All inputs are finite; a program needn't handle non-finite values.
Results may differ from the reference program's by a relative error of at most 0.0003.
Values may be sent and summed in bfloat16 or wider, within the bound.
A program may use at most 128 MiB of HBM per device.

```python
import math
import jax
import jax.numpy as jnp
from jax import lax

FEATURES = 1024
OUTPUTS = 32
BINS = 64
NODES = 8
ROWS = 49152


def plant(values, stream_key, smallest, high):
    place = [jax.random.randint(jax.random.fold_in(stream_key, axis), (), 0, length) for axis, length in enumerate(values.shape)]
    longest = values.shape.index(max(values.shape))
    beside = place[:longest] + [(place[longest] + 1) % values.shape[longest]] + place[longest + 1:]
    return values.at[tuple(place)].set(smallest).at[tuple(beside)].set(high)


def steps_of(key, dims, split, smallest, high):
    loudness, own = 1.0, jax.random.fold_in(key, 6)
    for position, blocks in split:
        draws = jnp.exp(jax.random.uniform(jax.random.fold_in(own, position), (blocks,), jnp.float32, smallest / len(split), high / len(split)))
        loudness = loudness * jnp.repeat(draws, dims[position] // blocks).reshape([-1 if axis == position else 1 for axis in range(len(dims))])
    return loudness


def normal_values(stream_key, extent, deviation, limit, split=(), held_as=jnp.bfloat16):
    values = jax.random.normal(stream_key, extent, jnp.float32) * deviation
    if len(split) > 0:
        values = steps_of(stream_key, extent, split, -0.22, 0.18) * values
    return jnp.clip(values, min=-limit, max=limit).astype(held_as)


def setup_inputs(seed: int = 0) -> dict:
    key_list = jax.random.split(jax.random.key(seed), 5)
    bin_index = plant(jax.random.randint(key_list[0], (FEATURES, ROWS), 0, BINS), jax.random.fold_in(key_list[0], 1), 0, BINS - 1).astype(jnp.int32)
    gradient = normal_values(key_list[1], (OUTPUTS, ROWS), 1.0, 6.0, ((1, 32),))
    hessian = jnp.clip(jnp.exp(math.log(4.0) - 2.7725887 * jax.random.uniform(key_list[2], (ROWS,), jnp.float32) ** steps_of(key_list[2], (ROWS,), ((0, 32),), -0.2, 0.2)), 0.25, 4.0).astype(jnp.bfloat16)
    row_node = plant(jax.random.randint(key_list[3], (ROWS,), 0, NODES), jax.random.fold_in(key_list[3], 1), 0, NODES - 1).astype(jnp.int32)
    return {"bin_index": bin_index, "gradient": gradient, "hessian": hessian, "row_node": row_node}


ridge_term = 1.0


def score_splits(histogram, whole_sums):
    left_sums = jnp.cumsum(histogram, axis=1)
    right_sums = whole_sums - left_sums

    def part_score(sums):
        return jnp.sum(sums[..., :-1] * sums[..., :-1], axis=-1) / (sums[..., -1] + ridge_term)

    outputs_count = histogram.shape[-1] - 1
    score_terms = part_score(left_sums) + part_score(right_sums) - part_score(whole_sums)
    return jnp.transpose((0.5 / outputs_count) * score_terms, (0, 2, 1))


def reference(bin_index, gradient, hessian, row_node):
    stacked = jnp.concatenate([gradient, hessian[None, :]], 0)
    stacked_rows = stacked.astype(jnp.float32).T
    node_ids = row_node.astype(jnp.int32)
    node_totals = jax.ops.segment_sum(stacked_rows, node_ids, num_segments=NODES)

    def one_feature(feature_bins):
        cell_ids = (node_ids * BINS + feature_bins.astype(jnp.int32)).astype(jnp.int32)
        sums = jax.ops.segment_sum(stacked_rows, cell_ids, num_segments=NODES * BINS)
        return jnp.transpose(sums.reshape(NODES, BINS, -1), (1, 0, 2))

    histogram = lax.map(one_feature, bin_index)
    split_gain = score_splits(histogram, node_totals[None, None])
    best_gain = jnp.max(split_gain, axis=(0, 2))
    return split_gain.reshape(FEATURES, NODES * BINS), best_gain
```

```python
import functools
import math

import jax
import jax.numpy as jnp
from jax import lax
from jax.experimental import pallas as pl
from jax.experimental.pallas import tpu as pltpu
from jax.sharding import PartitionSpec as P

BINS = 64
NODES = 8
GROUP = 8
PLANE = 4
LANES = 128
MESH = pl.DeviceIdType.MESH

ridge_term = 1.0


def flip(index, step, size):
    out, bit = 0, 1
    while bit < size:
        out = out + ((index // bit + step // bit) % 2) * bit
        bit *= 2
    return out


def send_plan(rows, plane):
    near = [t for t in range(plane, rows) if t % plane < plane // 2]
    far = [t for t in range(plane, rows) if t % plane >= plane // 2]
    first = near[: len(near) // 2 + 1]
    late = [t for t in near if t not in first] + far
    plan = {-1: list(range(1, plane)) + first}
    for i, t in enumerate(late):
        plan.setdefault(min(i, t - 1), []).append(t)
    return plan


def kernel(
    sizes,
    bins_ref,
    mine_ref,
    gain_ref,
    best_ref,
    raw,
    sent,
    got,
    stats,
    masked,
    sums,
    top,
    tops,
    load_sem,
    bin_send,
    bin_recv,
    stat_send,
    stat_recv,
    top_send,
    top_recv,
):
    rows, feats, plane, outputs_count, width = sizes
    owned, shard_rows = got.shape[1], got.shape[2]
    group = math.gcd(owned, GROUP)
    span = math.gcd(owned, 2 * group)
    columns = group * BINS
    planes = rows // plane
    r, y = lax.axis_index("row"), lax.axis_index("feat")

    def device(step, turn):
        return {"row": flip(r, step, rows), "feat": (y + turn) % feats}

    def load(t):
        d = flip(r, t, rows)
        return pltpu.make_async_copy(
            bins_ref.at[pl.ds(pl.multiple_of(d * owned, owned), owned)], raw.at[t], load_sem.at[t]
        )

    def bins_copy(t):
        return pltpu.make_async_remote_copy(
            src_ref=sent.at[t],
            dst_ref=got.at[t],
            send_sem=bin_send.at[t],
            recv_sem=bin_recv.at[t],
            device_id=device(t, 0),
            device_id_type=MESH,
        )

    def stat_copy(src, out_slot, in_slot, step, turn):
        return pltpu.make_async_remote_copy(
            src_ref=src,
            dst_ref=stats.at[in_slot],
            send_sem=stat_send.at[out_slot],
            recv_sem=stat_recv.at[in_slot],
            device_id=device(step, turn),
            device_id_type=MESH,
        )

    beside = [(i, v) for v in range(feats) for i in range(plane) if (i, v) != (0, 0)]

    def spread(src, base):
        for i, v in beside:
            stat_copy(
                src, (base + i) * feats + v, (base + i) * feats + (feats - v) % feats, i, v
            ).start()

    for t in range(rows):
        load(t).start()

    barrier = pltpu.get_barrier_semaphore()
    partners = [(t, 0) for t in range(1, rows)]
    partners += [(i, v) for v in range(1, feats) for i in range(plane)]
    for t, v in partners:
        pl.semaphore_signal(barrier, inc=1, device_id=device(t, v), device_id_type=MESH)

    def convert(t, _):
        load(t).wait()
        sent[t] = raw[t].astype(jnp.float32).astype(jnp.bfloat16)
        return 0

    lax.fori_loop(1, rows, convert, 0)
    load(0).wait()
    got[0] = raw[0].astype(jnp.float32).astype(jnp.bfloat16)
    stats[0] = mine_ref[...]
    sums[...] = jnp.zeros_like(sums)
    pl.semaphore_wait(barrier, len(partners))

    for p in range(1, planes):
        stat_copy(mine_ref, p * plane * feats, p * plane * feats, p * plane, 0).start()
    spread(mine_ref, 0)
    plan = send_plan(rows, plane)
    for t in plan[-1]:
        bins_copy(t).start()

    bin_levels = lax.broadcasted_iota(jnp.int32, (BINS, 1), 0).astype(jnp.bfloat16)
    node_levels = lax.broadcasted_iota(jnp.int32, (NODES, 1), 0).astype(jnp.float32)
    one, zero = jnp.bfloat16(1), jnp.bfloat16(0)
    tiles = width // LANES

    def step_of(t, _):
        @pl.when(t < planes - 1)
        def _():
            base = (t + 1) * plane
            slot = base * feats
            stat_copy(mine_ref, slot, slot, 0, 0).wait_recv()
            spread(stats.at[slot], base)

        for at, leaving in plan.items():
            if at >= 0:

                @pl.when(t == at)
                def _():
                    for other in leaving:
                        bins_copy(other).start()

        @pl.when(t > 0)
        def _():
            bins_copy(t).wait_recv()

        for u in range(feats):

            @pl.when((t % plane) + u > 0)
            def _():
                slot = t * feats + u
                stat_copy(mine_ref, slot, slot, 0, 0).wait_recv()

        for c in range(feats):
            chunk = stats.at[t * feats + (c + feats - y) % feats]
            extra = chunk[:, width : width + LANES]
            hess = jnp.concatenate([extra[j : j + 1] for j in range(tiles)], 1)
            node = jnp.concatenate([extra[tiles + j : tiles + j + 1] for j in range(tiles)], 1)
            grads = chunk[:, :width]
            where = slice(c * width, (c + 1) * width)
            for n in range(NODES):
                masked[n * outputs_count : (n + 1) * outputs_count, where] = jnp.where(
                    node == jnp.bfloat16(n), grads, zero
                )
            masked[NODES * outputs_count :, where] = jnp.where(
                node.astype(jnp.float32) == node_levels, hess.astype(jnp.float32), 0.0
            ).astype(jnp.bfloat16)

        def groups(trip, _):
            bins = got[t, pl.ds(pl.multiple_of(trip * span, span), span), :]
            for h in range(span // group):
                below = jnp.concatenate(
                    [
                        jnp.where(bins[j : j + 1] <= bin_levels, one, zero)
                        for j in range(h * group, (h + 1) * group)
                    ],
                    0,
                )
                sums[trip * (span // group) + h] += lax.dot_general(
                    masked[...], below, (((1,), (1,)), ((), ())), preferred_element_type=jnp.float32
                )
            return 0

        lax.fori_loop(0, owned // span, groups, 0)
        return 0

    lax.fori_loop(0, rows, step_of, 0)

    whole = sums[0, :, BINS - 1 : BINS]
    most = None
    for g in range(owned // group):
        lefts, rights, wholes = [], [], []
        for n in range(NODES):
            part = slice(n * outputs_count, (n + 1) * outputs_count)
            left = sums[g, part, :]
            right = whole[part] - left
            lefts.append(jnp.sum(left * left, 0, keepdims=True))
            rights.append(jnp.sum(right * right, 0, keepdims=True))
            wholes.append(jnp.sum(whole[part] * whole[part], 0, keepdims=True))
        left_hess = sums[g, NODES * outputs_count :, :]
        whole_hess = whole[NODES * outputs_count :]
        gain = (0.5 / outputs_count) * (
            jnp.concatenate(lefts, 0) / (left_hess + ridge_term)
            + jnp.concatenate(rights, 0) / (whole_hess - left_hess + ridge_term)
            - jnp.concatenate(wholes, 0) / (whole_hess + ridge_term)
        )
        gain_ref[:, g * columns : (g + 1) * columns] = gain
        for k in range(columns // LANES):
            tile = gain[:, k * LANES : (k + 1) * LANES]
            most = tile if most is None else jnp.maximum(most, tile)

    def top_copy(src, slot, step, turn, back):
        return pltpu.make_async_remote_copy(
            src_ref=top.at[src],
            dst_ref=tops.at[back],
            send_sem=top_send.at[slot],
            recv_sem=top_recv.at[back],
            device_id=device(step, turn),
            device_id_type=MESH,
        )

    top[0] = most
    across = [(rows + v, v, rows + feats - v) for v in range(1, feats)]
    for slot, v, back in across:
        top_copy(0, slot, 0, v, back).start()
    for slot, v, back in across:
        top_copy(0, slot, 0, v, slot).wait_recv()
        most = jnp.maximum(most, tops[slot])
    top[1] = most
    for t in range(1, rows):
        top_copy(1, t, t, 0, t).start()
    for t in range(1, rows):
        top_copy(1, t, t, 0, t).wait_recv()
        most = jnp.maximum(most, tops[t])
    best_ref[...] = jnp.broadcast_to(jnp.max(most, axis=1, keepdims=True), best_ref.shape)

    def drain_bins(t, _):
        bins_copy(t).wait_send()
        top_copy(1, t, t, 0, t).wait_send()
        return 0

    lax.fori_loop(1, rows, drain_bins, 0)
    for slot, v, back in across:
        top_copy(0, slot, 0, v, back).wait_send()

    def drain_stats(slot, _):
        stat_copy(mine_ref, slot, slot, 0, 0).wait_send()
        return 0

    lax.fori_loop(1, rows * feats, drain_stats, 0)


def on_device(bin_index, gradient, hessian, row_node):
    rows, feats = lax.axis_size("row"), lax.axis_size("feat")
    plane = math.gcd(rows, PLANE)
    owned = bin_index.shape[0] // rows
    outputs_count, width = gradient.shape
    shard_rows = bin_index.shape[1]
    channels = outputs_count + 1
    group = math.gcd(owned, GROUP)
    tiles = width // LANES
    nodes = lax.dynamic_slice_in_dim(row_node, lax.axis_index("feat") * width, width, 0)
    extra = jnp.concatenate(
        [hessian.reshape(tiles, LANES), nodes.astype(jnp.bfloat16).reshape(tiles, LANES)], 0
    )
    extra = jnp.pad(extra, ((0, outputs_count - 2 * tiles), (0, 0)))
    mine = jnp.concatenate([gradient, extra], 1)
    sizes = (rows, feats, plane, outputs_count, width)
    flops = 2 * channels * NODES * owned * BINS * rows * shard_rows
    vmem = pl.BlockSpec(memory_space=pltpu.VMEM)
    dma = pltpu.SemaphoreType.DMA
    gain, best = pl.pallas_call(
        functools.partial(kernel, sizes),
        out_shape=(
            jax.ShapeDtypeStruct((NODES, owned * BINS), jnp.float32),
            jax.ShapeDtypeStruct((NODES, LANES), jnp.float32),
        ),
        in_specs=[pl.BlockSpec(memory_space=pl.ANY), vmem],
        out_specs=(vmem, vmem),
        scratch_shapes=[
            pltpu.VMEM((rows, owned, shard_rows), jnp.int32),
            pltpu.VMEM((rows, owned, shard_rows), jnp.bfloat16),
            pltpu.VMEM((rows, owned, shard_rows), jnp.bfloat16),
            pltpu.VMEM((rows * feats, outputs_count, width + LANES), jnp.bfloat16),
            pltpu.VMEM((channels * NODES, shard_rows), jnp.bfloat16),
            pltpu.VMEM((owned // group, channels * NODES, group * BINS), jnp.float32),
            pltpu.VMEM((2, NODES, LANES), jnp.float32),
            pltpu.VMEM((rows + feats, NODES, LANES), jnp.float32),
            dma((rows,)),
            dma((rows,)),
            dma((rows,)),
            dma((rows * feats,)),
            dma((rows * feats,)),
            dma((rows + feats,)),
            dma((rows + feats,)),
        ],
        compiler_params=pltpu.CompilerParams(
            collective_id=1, has_side_effects=True, vmem_limit_bytes=56 * 1024 * 1024
        ),
        cost_estimate=pl.CostEstimate(
            flops=flops, bytes_accessed=4 * bin_index.size, transcendentals=0
        ),
        name="split_gains",
    )(bin_index, mine)
    split_gain = gain.reshape(NODES, owned, BINS).transpose(1, 0, 2)
    return (split_gain.reshape(owned, NODES * BINS), best[:, 0])


def solution(mesh):
    in_specs = (P("feat", "row"), P(None, ("row", "feat")), P(("row", "feat")), P("row"))
    out_specs = (P(("feat", "row"), None), P())
    return jax.shard_map(
        on_device, mesh=mesh, in_specs=in_specs, out_specs=out_specs, check_vma=False
    )
```

```python
import functools
import math

import jax
import jax.numpy as jnp
from jax import lax
from jax.experimental import pallas as pl
from jax.experimental.pallas import tpu as pltpu
from jax.sharding import PartitionSpec as P

BINS = 64
NODES = 8
GROUP = 8
PLANE = 4
LANES = 128
MESH = pl.DeviceIdType.MESH

ridge_term = 1.0


def flip(index, step, size):
    out, bit = 0, 1
    while bit < size:
        out = out + ((index // bit + step // bit) % 2) * bit
        bit *= 2
    return out


def send_plan(rows, plane):
    plan = {-1: list(range(1, plane))}
    for t in range(plane, rows):
        ring, close = t // plane, t % plane < max(plane // 2, 1)
        at = max(ring - 3, -1 if ring < 3 else 0) if close else 2 * ring - 1
        plan.setdefault(at, []).append(t)
    return plan


def kernel(
    sizes,
    bins_ref,
    grad_ref,
    hess_ref,
    node_ref,
    gain_ref,
    best_ref,
    raw,
    sent,
    got,
    stats,
    masked_even,
    masked_odd,
    sums,
    top,
    tops,
    load_sem,
    bin_send,
    bin_recv,
    stat_send,
    stat_recv,
    top_send,
    top_recv,
):
    rows, feats, plane, outputs_count, width = sizes
    owned, shard_rows = got.shape[1], got.shape[2]
    group = math.gcd(owned, GROUP)
    columns = group * BINS
    half, tiles = outputs_count // 2, width // LANES
    planes = rows // plane
    r, y = lax.axis_index("row"), lax.axis_index("feat")

    def device(step, turn):
        return {"row": flip(r, step, rows), "feat": (y + turn) % feats}

    def load(t):
        d = flip(r, t, rows)
        return pltpu.make_async_copy(
            bins_ref.at[pl.ds(pl.multiple_of(d * owned, owned), owned)], raw.at[t], load_sem.at[t]
        )

    def bins_copy(t):
        return pltpu.make_async_remote_copy(
            src_ref=sent.at[t],
            dst_ref=got.at[t],
            send_sem=bin_send.at[t],
            recv_sem=bin_recv.at[t],
            device_id=device(t, 0),
            device_id_type=MESH,
        )

    def stat_copy(src, out_slot, in_slot, step, turn):
        return pltpu.make_async_remote_copy(
            src_ref=src,
            dst_ref=stats.at[in_slot],
            send_sem=stat_send.at[out_slot],
            recv_sem=stat_recv.at[in_slot],
            device_id=device(step, turn),
            device_id_type=MESH,
        )

    pair = 2 - plane % 2
    beside = [(i, v) for v in range(feats) for i in range(0, plane, pair) if (i, v) != (0, 0)]

    def spread(src, base):
        for i, v in beside:
            stat_copy(
                src, (base + i) * feats + v, (base + i) * feats + (feats - v) % feats, i, v
            ).start()

    def share(src, slot):
        stat_copy(src, slot + feats, slot + feats, 1, 0).start()

    for t in range(rows):
        load(t).start()

    stats[0, :, :width] = grad_ref[...]
    stats[0, :, width:] = jnp.zeros((outputs_count, LANES), jnp.bfloat16)
    stats[0, :tiles, width:] = hess_ref[...]
    held = node_ref[:tiles]
    for c in range(1, feats):
        held = jnp.where(y == c, node_ref[c * tiles : (c + 1) * tiles], held)
    stats[0, half : half + tiles, width:] = held.astype(jnp.float32).astype(jnp.bfloat16)

    barrier = pltpu.get_barrier_semaphore()
    partners = [(t, 0) for t in range(1, rows)]
    partners += [(t, v) for v in range(1, feats) for t in range(rows)]
    for t, v in partners:
        pl.semaphore_signal(barrier, inc=1, device_id=device(t, v), device_id_type=MESH)

    plan = send_plan(rows, plane)
    early = max(plan[-1]) + 1

    def convert(t, _):
        load(t).wait()
        sent[t] = raw[t].astype(jnp.float32).astype(jnp.bfloat16)
        return 0

    pl.semaphore_wait(barrier, len(partners))
    for p in range(1, planes):
        stat_copy(stats.at[0], p * plane * feats, p * plane * feats, p * plane, 0).start()
    spread(stats.at[0], 0)
    if pair == 2:
        share(stats.at[0], 0)
    lax.fori_loop(1, early, convert, 0)
    for t in plan[-1]:
        bins_copy(t).start()
    load(0).wait()
    got[0] = raw[0].astype(jnp.float32).astype(jnp.bfloat16)
    lax.fori_loop(early, rows, convert, 0)
    sums[...] = jnp.zeros_like(sums)

    bin_levels = lax.broadcasted_iota(jnp.int32, (BINS, 1), 0).astype(jnp.bfloat16)
    node_levels = lax.broadcasted_iota(jnp.int32, (NODES, 1), 0).astype(jnp.float32)
    one, zero = jnp.bfloat16(1), jnp.bfloat16(0)

    def arrive(t):
        for u in range(feats):
            slot = t * feats + u

            @pl.when((t % plane) + u > 0)
            def _():
                stat_copy(stats.at[0], slot, slot, 0, 0).wait_recv()

            if pair == 2:

                @pl.when((t % 2 == 0) & (t + u > 0))
                def _():
                    share(stats.at[slot], slot)

    def mask(t, masked):
        for c in range(feats):
            chunk = stats.at[t * feats + (c + feats - y) % feats]
            extra = chunk[:, width : width + LANES]
            hess = jnp.concatenate([extra[j : j + 1] for j in range(tiles)], 1)
            node = jnp.concatenate([extra[half + j : half + j + 1] for j in range(tiles)], 1)
            grads = chunk[:, :width]
            where = slice(c * width, (c + 1) * width)
            for n in range(NODES):
                masked[n * outputs_count : (n + 1) * outputs_count, where] = jnp.where(
                    node == jnp.bfloat16(n), grads, zero
                )
            masked[NODES * outputs_count :, where] = jnp.where(
                node.astype(jnp.float32) == node_levels, hess.astype(jnp.float32), 0.0
            ).astype(jnp.bfloat16)

    def shard_of(t):
        rest = planes - 2
        if plane != PLANE or rest < 1:
            return t
        i, c = t // 2, t % 2
        late = 1 - (4 // (i + 1) + 3) // 4
        j = i + 4 * rest - 4
        return 2 * (i * (1 - late) + late * (4 + 2 * (j % rest) + j // rest - 4)) + c

    def step_of(t, masked, following):
        for p in range(1, planes):

            @pl.when(t == 2 * (p - 1))
            def _():
                slot = p * plane * feats
                stat_copy(stats.at[0], slot, slot, 0, 0).wait_recv()
                spread(stats.at[slot], p * plane)

        for at, leaving in plan.items():
            if at >= 0:

                @pl.when(t == at)
                def _():
                    for other in leaving:
                        bins_copy(other).start()

        @pl.when(t < rows - 1)
        def _():
            arrive(shard_of(t + 1))

        shard = shard_of(t)

        @pl.when(t > 0)
        def _():
            bins_copy(shard).wait_recv()

        mask(shard_of((t + 1) % rows), following)
        for g in range(owned // group):
            below = jnp.concatenate(
                [
                    jnp.where(got[shard, j : j + 1, :] <= bin_levels, one, zero)
                    for j in range(g * group, (g + 1) * group)
                ],
                0,
            )
            sums[g] += lax.dot_general(
                masked[...], below, (((1,), (1,)), ((), ())), preferred_element_type=jnp.float32
            )

    def two_steps(i, _):
        step_of(2 * i, masked_even, masked_odd)
        step_of(2 * i + 1, masked_odd, masked_even)
        return 0

    arrive(0)
    mask(0, masked_even)
    lax.fori_loop(0, rows // 2, two_steps, 0)

    whole = sums[0, :, BINS - 1 : BINS]
    most = None
    for g in range(owned // group):
        lefts, rights, wholes = [], [], []
        for n in range(NODES):
            part = slice(n * outputs_count, (n + 1) * outputs_count)
            left = sums[g, part, :]
            right = whole[part] - left
            lefts.append(jnp.sum(left * left, 0, keepdims=True))
            rights.append(jnp.sum(right * right, 0, keepdims=True))
            wholes.append(jnp.sum(whole[part] * whole[part], 0, keepdims=True))
        left_hess = sums[g, NODES * outputs_count :, :]
        whole_hess = whole[NODES * outputs_count :]
        gain = (0.5 / outputs_count) * (
            jnp.concatenate(lefts, 0) / (left_hess + ridge_term)
            + jnp.concatenate(rights, 0) / (whole_hess - left_hess + ridge_term)
            - jnp.concatenate(wholes, 0) / (whole_hess + ridge_term)
        )
        gain_ref[:, g * columns : (g + 1) * columns] = gain
        for k in range(columns // LANES):
            tile = gain[:, k * LANES : (k + 1) * LANES]
            most = tile if most is None else jnp.maximum(most, tile)

    def top_copy(t, v):
        back = t * feats + (feats - v) % feats
        return pltpu.make_async_remote_copy(
            src_ref=top,
            dst_ref=tops.at[back],
            send_sem=top_send.at[t * feats + v],
            recv_sem=top_recv.at[back],
            device_id=device(t, v),
            device_id_type=MESH,
        )

    top[...] = most
    for t, v in partners:
        top_copy(t, v).start()
    for t, v in partners:
        top_copy(t, (feats - v) % feats).wait_recv()
        most = jnp.maximum(most, tops[t * feats + v])
    most = jnp.broadcast_to(jnp.max(most, axis=1, keepdims=True), most.shape)
    across = lax.broadcasted_iota(jnp.int32, most.shape, 1)
    down = lax.broadcasted_iota(jnp.int32, most.shape, 0)
    best_ref[...] = jnp.sum(jnp.where(across == down, most, 0.0), 0, keepdims=True)[:, :NODES]

    def drain_bins(t, _):
        bins_copy(t).wait_send()
        return 0

    lax.fori_loop(1, rows, drain_bins, 0)
    for t, v in partners:
        top_copy(t, v).wait_send()

    def drain_stats(slot, _):
        stat_copy(stats.at[0], slot, slot, 0, 0).wait_send()
        return 0

    lax.fori_loop(1, rows * feats, drain_stats, 0)


def on_device(bin_index, gradient, hessian, row_node):
    rows, feats = lax.axis_size("row"), lax.axis_size("feat")
    plane = math.gcd(rows, PLANE)
    owned = bin_index.shape[0] // rows
    outputs_count, width = gradient.shape
    shard_rows = bin_index.shape[1]
    channels = outputs_count + 1
    group = math.gcd(owned, GROUP)
    sizes = (rows, feats, plane, outputs_count, width)
    flops = 2 * channels * NODES * owned * BINS * rows * shard_rows
    vmem = pl.BlockSpec(memory_space=pltpu.VMEM)
    dma = pltpu.SemaphoreType.DMA
    gain, best = pl.pallas_call(
        functools.partial(kernel, sizes),
        out_shape=(
            jax.ShapeDtypeStruct((NODES, owned * BINS), jnp.float32),
            jax.ShapeDtypeStruct((1, NODES), jnp.float32),
        ),
        in_specs=[pl.BlockSpec(memory_space=pl.ANY), vmem, vmem, vmem],
        out_specs=(vmem, vmem),
        scratch_shapes=[
            pltpu.VMEM((rows, owned, shard_rows), jnp.int32),
            pltpu.VMEM((rows, owned, shard_rows), jnp.bfloat16),
            pltpu.VMEM((rows, owned, shard_rows), jnp.bfloat16),
            pltpu.VMEM((rows * feats, outputs_count, width + LANES), jnp.bfloat16),
            pltpu.VMEM((channels * NODES, shard_rows), jnp.bfloat16),
            pltpu.VMEM((channels * NODES, shard_rows), jnp.bfloat16),
            pltpu.VMEM((owned // group, channels * NODES, group * BINS), jnp.float32),
            pltpu.VMEM((NODES, LANES), jnp.float32),
            pltpu.VMEM((rows * feats, NODES, LANES), jnp.float32),
            dma((rows,)),
            dma((rows,)),
            dma((rows,)),
            dma((rows * feats,)),
            dma((rows * feats,)),
            dma((rows * feats,)),
            dma((rows * feats,)),
        ],
        compiler_params=pltpu.CompilerParams(
            collective_id=1, has_side_effects=True, vmem_limit_bytes=56 * 1024 * 1024
        ),
        cost_estimate=pl.CostEstimate(
            flops=flops, bytes_accessed=4 * bin_index.size, transcendentals=0
        ),
        name="split_gains",
    )(bin_index, gradient, hessian.reshape(-1, LANES), row_node.reshape(-1, LANES))
    split_gain = gain.reshape(NODES, owned, BINS).transpose(1, 0, 2)
    return (split_gain.reshape(owned, NODES * BINS), best[0])


def solution(mesh):
    in_specs = (P("feat", "row"), P(None, ("row", "feat")), P(("row", "feat")), P("row"))
    out_specs = (P(("feat", "row"), None), P())
    return jax.shard_map(
        on_device, mesh=mesh, in_specs=in_specs, out_specs=out_specs, check_vma=False
    )
```

```python
import functools
import math

import jax
import jax.numpy as jnp
from jax import lax
from jax.experimental import pallas as pl
from jax.experimental.pallas import tpu as pltpu
from jax.sharding import PartitionSpec as P

BINS = 64
NODES = 8
GROUP = 8
PLANE = 4
LANES = 128
MESH = pl.DeviceIdType.MESH

ridge_term = 1.0


def flip(index, step, size):
    out, bit = 0, 1
    while bit < size:
        out = out + ((index // bit + step // bit) % 2) * bit
        bit *= 2
    return out


def send_plan(rows, plane):
    plan = {-1: list(range(1, plane))}
    for t in range(plane, rows):
        ring, close = t // plane, t % plane < max(plane // 2, 1)
        at = max(ring - 3, -1 if ring < 3 else 0) if close else 2 * ring - 1
        plan.setdefault(at, []).append(t)
    return plan


def parts_of(owned):
    return 2 if owned % 32 == 0 else 1


def kernel(
    sizes,
    bins_ref,
    grad_ref,
    hess_ref,
    node_ref,
    gain_ref,
    best_ref,
    raw,
    sent,
    got,
    stats,
    masked_even,
    masked_odd,
    sums,
    top,
    tops,
    load_sem,
    bin_send,
    bin_recv,
    stat_send,
    stat_recv,
    relay_send,
    top_send,
    top_recv,
):
    rows, feats, plane, outputs_count, width = sizes
    owned, shard_rows = got.shape[1], got.shape[2]
    group = math.gcd(owned, GROUP)
    parts = parts_of(owned)
    columns = group * BINS
    half, tiles = outputs_count // 2, width // LANES
    planes = rows // plane
    r, y = lax.axis_index("row"), lax.axis_index("feat")

    def device(step, turn):
        return {"row": flip(r, step, rows), "feat": (y + turn) % feats}

    def load(t):
        d = flip(r, t, rows)
        return pltpu.make_async_copy(
            bins_ref.at[pl.ds(pl.multiple_of(d * owned, owned), owned)], raw.at[t], load_sem.at[t]
        )

    def bins_copy(t, h):
        piece = pl.ds(h * (owned // parts), owned // parts)
        return pltpu.make_async_remote_copy(
            src_ref=sent.at[t, piece],
            dst_ref=got.at[t, piece],
            send_sem=bin_send.at[t * parts + h],
            recv_sem=bin_recv.at[t * parts + h],
            device_id=device(t, 0),
            device_id_type=MESH,
        )

    def send_bins(t):
        for h in range(parts):
            bins_copy(t, h).start()

    def stat_copy(src, out_slot, in_slot, step, turn):
        return pltpu.make_async_remote_copy(
            src_ref=src,
            dst_ref=stats.at[in_slot],
            send_sem=stat_send.at[out_slot],
            recv_sem=stat_recv.at[in_slot],
            device_id=device(step, turn),
            device_id_type=MESH,
        )

    pair = 2 - plane % 2
    beside = [(i, v) for v in range(feats) for i in range(0, plane, pair) if (i, v) != (0, 0)]

    def spread(src, base):
        for i, v in beside:
            stat_copy(
                src, (base + i) * feats + v, (base + i) * feats + (feats - v) % feats, i, v
            ).start()

    def share(src, slot):
        stat_copy(src, slot + feats, slot + feats, 1, 0).start()

    plan = send_plan(rows, plane)
    first = sorted(plan[-1], key=lambda t: (t < plane, t))
    rest = [t for t in range(1, rows) if t not in first]
    for t in first + [0] + rest:
        load(t).start()

    stats[0, :, :width] = grad_ref[...]
    stats[0, :, width:] = jnp.zeros((outputs_count, LANES), jnp.bfloat16)
    stats[0, :tiles, width:] = hess_ref[...]
    held = node_ref[:tiles]
    for c in range(1, feats):
        held = jnp.where(y == c, node_ref[c * tiles : (c + 1) * tiles], held)
    stats[0, half : half + tiles, width:] = held.astype(jnp.float32).astype(jnp.bfloat16)

    barrier = pltpu.get_barrier_semaphore()
    partners = [(t, 0) for t in range(1, rows)]
    partners += [(t, v) for v in range(1, feats) for t in range(rows)]
    for t, v in partners:
        pl.semaphore_signal(barrier, inc=1, device_id=device(t, v), device_id_type=MESH)

    def convert(t, _):
        load(t).wait()
        sent[t] = raw[t].astype(jnp.float32).astype(jnp.bfloat16)
        return 0

    def relay(p):
        slot = p * plane * feats
        return pltpu.make_async_remote_copy(
            src_ref=stats.at[0],
            dst_ref=stats.at[slot],
            send_sem=relay_send.at[p],
            recv_sem=stat_recv.at[slot],
            device_id=device(p * plane, 0),
            device_id_type=MESH,
        )

    def wait_ring(p):
        slot = p * plane * feats
        stat_copy(stats.at[0], slot, slot, 0, 0).wait_recv()

    pl.semaphore_wait(barrier, len(partners))
    for p in range(1, planes):
        relay(p).start()
    spread(stats.at[0], 0)
    if pair == 2:
        share(stats.at[0], 0)
    ahead = [t for t in first if t < plane]
    for i, t in enumerate(ahead):
        convert(t, 0)
        if i > 0:
            send_bins(ahead[i - 1])
    load(0).wait()
    got[0] = raw[0].astype(jnp.float32).astype(jnp.bfloat16)
    send_bins(ahead[-1])
    for t in first[: -len(ahead)] + rest:
        convert(t, 0)
    for t in first[: -len(ahead)]:
        send_bins(t)
    sums[...] = jnp.zeros_like(sums)

    bin_levels = lax.broadcasted_iota(jnp.int32, (BINS, 1), 0).astype(jnp.bfloat16)
    node_levels = lax.broadcasted_iota(jnp.int32, (NODES, 1), 0).astype(jnp.float32)
    one, zero = jnp.bfloat16(1), jnp.bfloat16(0)

    def arrive(t):
        for u in range(feats):
            slot = t * feats + u

            @pl.when((t % plane) + u > 0)
            def _():
                stat_copy(stats.at[0], slot, slot, 0, 0).wait_recv()

            if pair == 2:

                @pl.when((t % 2 == 0) & (t + u > 0))
                def _():
                    share(stats.at[slot], slot)

    def mask(t, masked):
        for c in range(feats):
            chunk = stats.at[t * feats + (c + feats - y) % feats]
            extra = chunk[:, width : width + LANES]
            hess = jnp.concatenate([extra[j : j + 1] for j in range(tiles)], 1)
            node = jnp.concatenate([extra[half + j : half + j + 1] for j in range(tiles)], 1)
            grads = chunk[:, :width]
            where = slice(c * width, (c + 1) * width)
            for n in range(NODES):
                masked[n * outputs_count : (n + 1) * outputs_count, where] = jnp.where(
                    node == jnp.bfloat16(n), grads, zero
                )
            masked[NODES * outputs_count :, where] = jnp.where(
                node.astype(jnp.float32) == node_levels, hess.astype(jnp.float32), 0.0
            ).astype(jnp.bfloat16)

    def shard_of(t):
        rest = planes - 2
        if plane != PLANE or rest < 1:
            return t
        i, c = t // 2, t % 2
        late = 1 - (4 // (i + 1) + 3) // 4
        j = i + 4 * rest - 4
        return 2 * (i * (1 - late) + late * (4 + 2 * (j % rest) + j // rest - 4)) + c

    def step_of(t, masked, following):
        for p in range(1, planes):

            @pl.when(t == 2 * (p - 1))
            def _():
                wait_ring(p)
                spread(stats.at[p * plane * feats], p * plane)

        for at, leaving in plan.items():
            if at >= 0:

                @pl.when(t == at)
                def _():
                    for other in leaving:
                        send_bins(other)

        @pl.when(t < rows - 1)
        def _():
            arrive(shard_of(t + 1))

        shard = shard_of(t)

        @pl.when(t > 0)
        def _():
            bins_copy(shard, 0).wait_recv()

        mask(shard_of((t + 1) % rows), following)
        for g in range(owned // group):
            if g > 0 and g * group % (owned // parts) == 0:

                @pl.when(t > 0)
                def _():
                    bins_copy(shard, g * group // (owned // parts)).wait_recv()

            below = jnp.concatenate(
                [
                    jnp.where(got[shard, j : j + 1, :] <= bin_levels, one, zero)
                    for j in range(g * group, (g + 1) * group)
                ],
                0,
            )
            sums[g] += lax.dot_general(
                masked[...], below, (((1,), (1,)), ((), ())), preferred_element_type=jnp.float32
            )

    def two_steps(i, _):
        step_of(2 * i, masked_even, masked_odd)
        step_of(2 * i + 1, masked_odd, masked_even)
        return 0

    arrive(0)
    mask(0, masked_even)
    lax.fori_loop(0, rows // 2, two_steps, 0)

    whole = sums[0, :, BINS - 1 : BINS]
    most = None
    for g in range(owned // group):
        lefts, rights, wholes = [], [], []
        for n in range(NODES):
            part = slice(n * outputs_count, (n + 1) * outputs_count)
            left = sums[g, part, :]
            right = whole[part] - left
            lefts.append(jnp.sum(left * left, 0, keepdims=True))
            rights.append(jnp.sum(right * right, 0, keepdims=True))
            wholes.append(jnp.sum(whole[part] * whole[part], 0, keepdims=True))
        left_hess = sums[g, NODES * outputs_count :, :]
        whole_hess = whole[NODES * outputs_count :]
        gain = (0.5 / outputs_count) * (
            jnp.concatenate(lefts, 0) / (left_hess + ridge_term)
            + jnp.concatenate(rights, 0) / (whole_hess - left_hess + ridge_term)
            - jnp.concatenate(wholes, 0) / (whole_hess + ridge_term)
        )
        for j in range(group):
            gain_ref[:, g * group + j, :] = gain[:, j * BINS : (j + 1) * BINS]
        for k in range(columns // LANES):
            tile = gain[:, k * LANES : (k + 1) * LANES]
            most = tile if most is None else jnp.maximum(most, tile)

    def top_copy(t, v):
        back = t * feats + (feats - v) % feats
        return pltpu.make_async_remote_copy(
            src_ref=top,
            dst_ref=tops.at[back],
            send_sem=top_send.at[t * feats + v],
            recv_sem=top_recv.at[back],
            device_id=device(t, v),
            device_id_type=MESH,
        )

    most = jnp.broadcast_to(jnp.max(most, axis=1, keepdims=True), most.shape)
    across = lax.broadcasted_iota(jnp.int32, most.shape, 1)
    down = lax.broadcasted_iota(jnp.int32, most.shape, 0)
    most = jnp.sum(jnp.where(across == down, most, 0.0), 0, keepdims=True)
    top[...] = most
    for t, v in sorted(partners, reverse=True):
        top_copy(t, v).start()
    for t, v in partners:
        top_copy(t, (feats - v) % feats).wait_recv()
        most = jnp.maximum(most, tops[t * feats + v])
    best_ref[...] = most[:, :NODES]

    def drain_bins(t, _):
        for h in range(parts):
            bins_copy(t, h).wait_send()
        return 0

    lax.fori_loop(1, rows, drain_bins, 0)
    for t, v in partners:
        top_copy(t, v).wait_send()

    for i, v in beside:
        for p in range(planes):
            slot = (p * plane + i) * feats + v
            stat_copy(stats.at[0], slot, slot, 0, 0).wait_send()
    if pair == 2:
        for t in range(1, rows, 2):
            for u in range(feats):
                stat_copy(stats.at[0], t * feats + u, t * feats + u, 0, 0).wait_send()
    for p in range(1, planes):
        relay(p).wait_send()


def on_device(bin_index, gradient, hessian, row_node):
    rows, feats = lax.axis_size("row"), lax.axis_size("feat")
    plane = math.gcd(rows, PLANE)
    owned = bin_index.shape[0] // rows
    outputs_count, width = gradient.shape
    shard_rows = bin_index.shape[1]
    channels = outputs_count + 1
    group = math.gcd(owned, GROUP)
    sizes = (rows, feats, plane, outputs_count, width)
    flops = 2 * channels * NODES * owned * BINS * rows * shard_rows
    vmem = pl.BlockSpec(memory_space=pltpu.VMEM)
    dma = pltpu.SemaphoreType.DMA
    gain, best = pl.pallas_call(
        functools.partial(kernel, sizes),
        out_shape=(
            jax.ShapeDtypeStruct((NODES, owned, BINS), jnp.float32),
            jax.ShapeDtypeStruct((1, NODES), jnp.float32),
        ),
        in_specs=[pl.BlockSpec(memory_space=pl.ANY), vmem, vmem, vmem],
        out_specs=(vmem, vmem),
        scratch_shapes=[
            pltpu.VMEM((rows, owned, shard_rows), jnp.int32),
            pltpu.VMEM((rows, owned, shard_rows), jnp.bfloat16),
            pltpu.VMEM((rows, owned, shard_rows), jnp.bfloat16),
            pltpu.VMEM((rows * feats, outputs_count, width + LANES), jnp.bfloat16),
            pltpu.VMEM((channels * NODES, shard_rows), jnp.bfloat16),
            pltpu.VMEM((channels * NODES, shard_rows), jnp.bfloat16),
            pltpu.VMEM((owned // group, channels * NODES, group * BINS), jnp.float32),
            pltpu.VMEM((1, LANES), jnp.float32),
            pltpu.VMEM((rows * feats, 1, LANES), jnp.float32),
            dma((rows,)),
            dma((rows * parts_of(owned),)),
            dma((rows * parts_of(owned),)),
            dma((rows * feats,)),
            dma((rows * feats,)),
            dma((rows // plane,)),
            dma((rows * feats,)),
            dma((rows * feats,)),
        ],
        compiler_params=pltpu.CompilerParams(
            collective_id=1, has_side_effects=True, vmem_limit_bytes=56 * 1024 * 1024
        ),
        cost_estimate=pl.CostEstimate(
            flops=flops, bytes_accessed=4 * bin_index.size, transcendentals=0
        ),
        name="split_gains",
    )(bin_index, gradient, hessian.reshape(-1, LANES), row_node.reshape(-1, LANES))
    split_gain = gain.transpose(1, 0, 2)
    return (split_gain.reshape(owned, NODES * BINS), best[0])


def solution(mesh):
    in_specs = (P("feat", "row"), P(None, ("row", "feat")), P(("row", "feat")), P("row"))
    out_specs = (P(("feat", "row"), None), P())
    return jax.shard_map(
        on_device, mesh=mesh, in_specs=in_specs, out_specs=out_specs, check_vma=False
    )
```
